32 devices in a mesh: dp: 8 (over z, y), neg: 4 (over x, core).
Axes of the slice: x: 2, y: 2, z: 4, core: 2. Of those that a mesh axis runs over, the one named last changes fastest.
Arguments:
- query_features: bfloat16 [8192, 512], P(('dp', 'neg')), may hold values from -8 to 8
- positive_features: bfloat16 [8192, 512], P(('dp', 'neg')), may hold values from -6 to 6
- negative_features: bfloat16 [16384, 512], P(('neg', 'dp')), may hold values from -6 to 6
- positive_ids: int32 [8192], P('dp'), may hold values from 0 to 8191, as said below
- positive_counts: int32 [8192], P(('dp', 'neg')), may hold values from 1 to 16
- negative_ids: int32 [16384], P('neg'), may hold values from 0 to 4095, as said below
- negative_counts: int32 [16384], P('neg'), may hold values from 64 to 4096
- query_first: bfloat16 [512, 1024], replicated, may hold values from -0.25 to 0.25
- query_second: bfloat16 [1024, 512], replicated, may hold values from -0.1875 to 0.1875
- query_third: bfloat16 [512, 256], replicated, may hold values from -0.25 to 0.25
- item_first: bfloat16 [512, 1024], replicated, may hold values from -0.25 to 0.25
- item_second: bfloat16 [1024, 512], replicated, may hold values from -0.1875 to 0.1875
- item_third: bfloat16 [512, 256], replicated, may hold values from -0.25 to 0.25
Outputs:
- mean_loss: float32 [], replicated
- clipped_query_first: float32 [512, 1024], P('dp')
- clipped_query_second: float32 [1024, 512], P('dp')
- clipped_query_third: float32 [512, 256], P('dp')
- clipped_item_first: float32 [512, 1024], P('dp')
- clipped_item_second: float32 [1024, 512], P('dp')
- clipped_item_third: float32 [512, 256], P('dp')
The draws below stay inside these ranges and needn't reach their ends.
Inputs may be any that keep to these rules, and one draw needn't show every extreme that they name: `negative_ids`: ids of the sampled negatives; one id may stand for several negatives. `positive_ids`: A query's positive id may equal the ids of some negatives; those negatives are left out of that query's denominator.
All inputs are finite; a program needn't handle non-finite values.
Results may differ from the reference program's by a relative error of at most 0.0075.
Values may be sent and summed in bfloat16 or wider, within the bound.
No kernel may reach another device: no remote copies, remote signals or barrier semaphores. Data moves between devices by JAX's collectives and lax.ppermute only.
A program may use at most 128 MiB of HBM per device.

```python
import math
import jax
import jax.numpy as jnp
from jax import lax

FIN = 512
H1 = 1024
H2 = 512
E = 256
NEG = 16384
QUERIES = 8192


def draw_query_features(key, part):
    noise_key, mean_key, scale_key = jax.random.split(key, 3)
    values = jax.random.normal(noise_key, (QUERIES, FIN), jnp.float32)
    return jnp.clip(values, -8.0, 8.0).astype(jnp.bfloat16)


def draw_item_ids(key):
    base = jax.random.fold_in(key, 91)
    pool_key, pick_key, fresh_key, hit_key = jax.random.split(base, 4)
    negatives = jax.random.randint(pool_key, (NEG,), 0, NEG // 4, jnp.int32)
    negatives = negatives.at[0].set(NEG // 4 - 1).at[1].set(0)
    picked = jax.random.randint(pick_key, (QUERIES,), 0, NEG, jnp.int32)
    fresh = jax.random.randint(fresh_key, (QUERIES,), NEG // 4, NEG // 2, jnp.int32)
    choose_hit = jax.random.randint(hit_key, (QUERIES,), 0, 2, jnp.int32)
    positives = jnp.where(choose_hit == 0, negatives[picked], fresh)
    positives = positives.at[0].set(NEG // 2 - 1).at[1].set(0)
    return (negatives, positives)


def draw_negative_ids(key, part):
    return draw_item_ids(key)[0]


def draw_positive_ids(key, part):
    return draw_item_ids(key)[1]


def blocked_counts(key, total, block_rows, low_power, high_power):
    level_key, fine_key = jax.random.split(key)
    levels = jax.random.randint(level_key, (total // block_rows + 1,), low_power, high_power + 1, jnp.int32)
    powers = jnp.left_shift(jnp.ones_like(levels), levels)
    which = jnp.arange(total, dtype=jnp.int32) // block_rows
    base = powers[which]
    fine = jax.random.randint(fine_key, (total,), 0, 65536, jnp.int32) % base
    return base + fine


def draw_negative_counts(key, part):
    counts = blocked_counts(jax.random.fold_in(key, 17), NEG, 256, 6, 11)
    return counts.at[0].set(4096).at[1].set(64)


def draw_positive_counts(key, part):
    counts = blocked_counts(jax.random.fold_in(key, 23), QUERIES, 64, 0, 3)
    return counts.at[0].set(16).at[1].set(1)


def block_scale(key, shape, pieces, least, top_value):
    loudness = 1.0
    for dim, parts in pieces:
        heights = jax.random.uniform(jax.random.fold_in(jax.random.fold_in(key, 6), dim), (parts,), jnp.float32, least / len(pieces), top_value / len(pieces))
        loudness = loudness * jnp.repeat(jnp.exp(heights), shape[dim] // parts).reshape((-1,) + (1,) * (len(shape) - 1 - dim))
    return loudness


def bell_draw(key, shape, scale, limit, shards=(), kind=jnp.bfloat16):
    gain = block_scale(key, shape, shards, -0.22, 0.18) if shards else 1.0
    drawn = jax.random.normal(key, shape, jnp.float32) * scale * gain
    return jnp.minimum(jnp.maximum(drawn, -limit), limit).astype(kind)


def setup_inputs(seed: int = 0) -> dict:
    streams_of = jax.random.split(jax.random.key(seed), 14)
    query_features = draw_query_features(jax.random.fold_in(streams_of[13], 71), 0)
    positive_features = bell_draw(streams_of[1], (QUERIES, FIN), 1.0, 6.0, ((0, 32),))
    negative_features = bell_draw(streams_of[2], (NEG, FIN), 1.0, 6.0, ((0, 32),))
    positive_ids = draw_positive_ids(jax.random.fold_in(streams_of[13], 71), 0)
    positive_counts = draw_positive_counts(jax.random.fold_in(streams_of[13], 71), 0)
    negative_ids = draw_negative_ids(jax.random.fold_in(streams_of[13], 71), 0)
    negative_counts = draw_negative_counts(jax.random.fold_in(streams_of[13], 71), 0)
    query_first = bell_draw(streams_of[7], (FIN, H1), FIN ** -0.5, 0.25)
    query_second = bell_draw(streams_of[8], (H1, H2), H1 ** -0.5, 0.1875)
    query_third = bell_draw(streams_of[9], (H2, E), H2 ** -0.5, 0.25)
    item_first = bell_draw(streams_of[10], (FIN, H1), FIN ** -0.5, 0.25)
    item_second = bell_draw(streams_of[11], (H1, H2), H1 ** -0.5, 0.1875)
    item_third = bell_draw(streams_of[12], (H2, E), H2 ** -0.5, 0.25)
    return dict(query_features=query_features, positive_features=positive_features, negative_features=negative_features, positive_ids=positive_ids, positive_counts=positive_counts, negative_ids=negative_ids, negative_counts=negative_counts, query_first=query_first, query_second=query_second, query_third=query_third, item_first=item_first, item_second=item_second, item_third=item_third)


inv_temp = 20.0
clip_norm = 256.0

def silu_slope(pre):
    sigma = jax.nn.sigmoid(pre)
    return sigma * (1.0 + pre * (1.0 - sigma))

def contract_rows(left, right):
    return lax.dot_general(left, right, (((0,), (0,)), ((), ())), preferred_element_type=jnp.float32)

def contract_cols(left, right):
    return lax.dot_general(left, right, (((1,), (1,)), ((), ())), preferred_element_type=jnp.float32)

def tower_forward(features, first, second, third):
    first_pre = jnp.dot(features, first, preferred_element_type=jnp.float32)
    first_act = jax.nn.silu(first_pre).astype(jnp.bfloat16)
    second_pre = jnp.dot(first_act, second, preferred_element_type=jnp.float32)
    second_act = jax.nn.silu(second_pre).astype(jnp.bfloat16)
    embedding = jnp.dot(second_act, third, preferred_element_type=jnp.float32)
    inv_norm = lax.rsqrt(lax.optimization_barrier(jnp.sum(embedding * embedding, axis=1, keepdims=True)) + 1.0)
    unit = (embedding * inv_norm).astype(jnp.bfloat16)
    return ((first_pre, first_act, second_pre, second_act, embedding, inv_norm), unit)

def tower_backward(features, second, third, saved, unit_grad):
    first_pre, first_act, second_pre, second_act, embedding, inv_norm = saved
    along = lax.optimization_barrier(jnp.sum(embedding * unit_grad, axis=1, keepdims=True))
    embed_grad = (inv_norm * unit_grad - inv_norm * inv_norm * inv_norm * embedding * along).astype(jnp.bfloat16)
    third_grad = contract_rows(second_act, embed_grad)
    second_slope = (contract_cols(embed_grad, third) * silu_slope(second_pre)).astype(jnp.bfloat16)
    second_grad = contract_rows(first_act, second_slope)
    first_slope = (contract_cols(second_slope, second) * silu_slope(first_pre)).astype(jnp.bfloat16)
    first_grad = contract_rows(features, first_slope)
    return (first_grad, second_grad, third_grad)

def reference(query_features, positive_features, negative_features, positive_ids, positive_counts, negative_ids, negative_counts, query_first, query_second, query_third, item_first, item_second, item_third):
    query_saved, query_unit = tower_forward(query_features, query_first, query_second, query_third)
    item_features = jnp.concatenate([positive_features, negative_features], axis=0)
    item_saved, item_unit = tower_forward(item_features, item_first, item_second, item_third)
    positive_unit = item_unit[:QUERIES]
    negative_unit = item_unit[QUERIES:]
    negative_log = jnp.log(negative_counts.astype(jnp.float32))
    positive_logit = lax.optimization_barrier(jnp.sum(query_unit.astype(jnp.float32) * positive_unit.astype(jnp.float32), axis=1)) * inv_temp - jnp.log(positive_counts.astype(jnp.float32))
    block_rows = math.gcd(QUERIES, 2048)
    blocks = QUERIES // block_rows

    def block_step(carry, inputs):
        negative_sum, loss_sum = carry
        query_block, positive_block, logit_block, ids_block = inputs
        scores = contract_cols(query_block, negative_unit) * inv_temp - negative_log[None, :]
        weights = jnp.where(ids_block[:, None] != negative_ids[None, :], jnp.exp(scores), 0.0)
        positive_exp = jnp.exp(logit_block)
        denom = positive_exp + lax.optimization_barrier(jnp.sum(weights, axis=1))
        loss_sum = loss_sum + jnp.sum(jnp.log(denom) - logit_block)
        softmax_weights = (weights / denom[:, None]).astype(jnp.bfloat16)
        positive_slope = positive_exp / denom - 1.0
        query_grad = (jnp.dot(softmax_weights, negative_unit, preferred_element_type=jnp.float32) + positive_slope[:, None] * positive_block.astype(jnp.float32)) * inv_temp
        positive_grad = positive_slope[:, None] * query_block.astype(jnp.float32) * inv_temp
        negative_sum = negative_sum + contract_rows(softmax_weights, query_block)
        return ((negative_sum, loss_sum), (query_grad, positive_grad))
    inputs = (query_unit.reshape(blocks, block_rows, E), positive_unit.reshape(blocks, block_rows, E), positive_logit.reshape(blocks, block_rows), positive_ids.reshape(blocks, block_rows))
    initial = (jnp.zeros((NEG, E), jnp.float32), jnp.zeros((), jnp.float32))
    (negative_sum, loss_sum), (query_grad, positive_grad) = lax.scan(block_step, initial, inputs)
    query_grad = query_grad.reshape(QUERIES, E)
    item_grad = jnp.concatenate([positive_grad.reshape(QUERIES, E), negative_sum * inv_temp], axis=0)
    query_grads = tower_backward(query_features, query_second, query_third, query_saved, query_grad)
    item_grads = tower_backward(item_features, item_second, item_third, item_saved, item_grad)
    gradients = query_grads + item_grads
    squares = jnp.zeros((), jnp.float32)
    for gradient in gradients:
        squares = squares + jnp.sum(gradient * gradient)
    grad_norm = jnp.sqrt(squares)
    clip_factor = clip_norm / jnp.maximum(grad_norm, clip_norm)
    mean_loss = loss_sum / QUERIES
    return (mean_loss, gradients[0] * clip_factor, gradients[1] * clip_factor, gradients[2] * clip_factor, gradients[3] * clip_factor, gradients[4] * clip_factor, gradients[5] * clip_factor)
```

```python
import jax
import jax.numpy as jnp
import numpy as np
from jax import lax
from jax.sharding import PartitionSpec as P


inv_temp = 20.0
clip_norm = 256.0
both = ("dp", "neg")
bf16 = jnp.bfloat16
f32 = jnp.float32


def silu_slope(pre):
    sigma = jax.nn.sigmoid(pre)
    return sigma * (1.0 + pre * (1.0 - sigma))


def contract_rows(left, right):
    return lax.dot_general(left, right, (((0,), (0,)), ((), ())), preferred_element_type=f32)


def contract_cols(left, right):
    return lax.dot_general(left, right, (((1,), (1,)), ((), ())), preferred_element_type=f32)


def tower_forward(features, first, second, third):
    first_pre = jnp.dot(features, first, preferred_element_type=f32)
    first_act = jax.nn.silu(first_pre).astype(bf16)
    second_pre = jnp.dot(first_act, second, preferred_element_type=f32)
    second_act = jax.nn.silu(second_pre).astype(bf16)
    embedding = jnp.dot(second_act, third, preferred_element_type=f32)
    inv_norm = lax.rsqrt(jnp.sum(embedding * embedding, axis=1, keepdims=True) + 1.0)
    unit = (embedding * inv_norm).astype(bf16)
    return ((first_pre, first_act, second_pre, second_act, embedding, inv_norm), unit)


def tower_backward(features, second, third, saved, unit_grad):
    first_pre, first_act, second_pre, second_act, embedding, inv_norm = saved
    along = jnp.sum(embedding * unit_grad, axis=1, keepdims=True)
    embed_grad = (inv_norm * unit_grad - inv_norm * inv_norm * inv_norm * embedding * along).astype(
        bf16
    )
    third_grad = contract_rows(second_act, embed_grad)
    second_slope = (contract_cols(embed_grad, third) * silu_slope(second_pre)).astype(bf16)
    second_grad = contract_rows(first_act, second_slope)
    first_slope = (contract_cols(second_slope, second) * silu_slope(first_pre)).astype(bf16)
    first_grad = contract_rows(features, first_slope)
    return (first_grad, second_grad, third_grad)


def swap(value, mask):
    devices = lax.axis_size("dp") * lax.axis_size("neg")
    return lax.ppermute(value, both, [(i, i ^ mask) for i in range(devices)])


def double(rows, masks):
    for mask in masks:
        rows = jnp.concatenate([rows, swap(rows, mask)], axis=0)
    return rows


def halve(rows, masks):
    for mask in reversed(masks):
        half = rows.shape[0] // 2
        rows = rows[:half] + swap(rows[half:].astype(bf16), mask).astype(f32)
    return rows


def keys_of(masks):
    keys = [0]
    for mask in masks:
        keys = keys + [key ^ mask for key in keys]
    return keys


def table_of(pairs):
    halves, keys = zip(*pairs)
    return np.array(halves, np.int32), np.array(keys, np.int32)


def pick_rows(table, rows):
    chosen = rows[:, None] == jnp.arange(table.shape[0])[None, :]
    return jnp.dot(
        chosen.astype(f32),
        table.astype(f32),
        precision=lax.Precision.HIGHEST,
        preferred_element_type=f32,
    )


def scatter_sum(array, bits, order, flat):
    alive = list(range(bits))
    for bit in order:
        axis = alive.index(bits - 1 - bit)
        own = (flat >> bit) & 1
        keep = lax.dynamic_index_in_dim(array, own, axis, keepdims=False)
        send = lax.dynamic_index_in_dim(array, 1 - own, axis, keepdims=False)
        array = keep + swap(send.astype(bf16), 1 << bit).astype(f32)
        alive.pop(axis)
    return array


def per_device(
    query_features,
    positive_features,
    negative_features,
    positive_ids,
    positive_counts,
    negative_ids,
    negative_counts,
    query_first,
    query_second,
    query_third,
    item_first,
    item_second,
    item_third,
):
    dps, negs = lax.axis_size("dp"), lax.axis_size("neg")
    devices = dps * negs
    bits = devices.bit_length() - 1
    neg_bits = negs.bit_length() - 1
    dp, neg = lax.axis_index("dp"), lax.axis_index("neg")
    flat = dp * negs + neg
    own_rows = query_features.shape[0]
    half_rows = own_rows // 2
    neg_rows = negative_features.shape[0]
    half_negs = neg_rows // 2

    core = 1
    across = [1 << k for k in range(1, neg_bits)]
    y_mask = negs
    plane_a, plane_b = across + [y_mask], [y_mask] + across
    line_a = [2 * negs << k for k in range(bits - neg_bits - 1)]
    if len(line_a) > 1:
        line_a[1] ^= line_a[0]
    line_b = line_a[::-1]

    keys_a, keys_b = keys_of(plane_a), keys_of(plane_b)
    blocks = [(0, k) for k in keys_a] + [(1, k) for k in keys_b]
    blocks = blocks + [(c, k ^ core) for c, k in blocks]
    ids_table = jnp.concatenate(
        [ids.reshape(2 * negs, half_rows) for ids in (positive_ids, swap(positive_ids, y_mask))], axis=0
    )
    part, key = table_of(blocks)
    block_rows = ((key // negs) & 1) * (2 * negs) + (neg ^ (key % negs)) * 2 + part
    group_ids = pick_rows(ids_table, block_rows).reshape(-1)

    lines = [(0, k) for k in keys_of(line_a)] + [(1, k) for k in keys_of(line_b)]
    part, key = table_of(lines)
    line_rows = (dp ^ (key // negs)) * 2 + part
    shard_ids = pick_rows(negative_ids.reshape(2 * dps, half_negs), line_rows).reshape(-1)
    shard_log = jnp.log(
        pick_rows(negative_counts.reshape(2 * dps, half_negs), line_rows).reshape(-1)
    )

    negative_saved, negative_unit = tower_forward(negative_features, item_first, item_second, item_third)
    shard_unit = jnp.concatenate(
        [double(negative_unit[:half_negs], line_a), double(negative_unit[half_negs:], line_b)], axis=0
    )
    query_saved, query_unit = tower_forward(query_features, query_first, query_second, query_third)
    group_unit = double(
        jnp.concatenate(
            [double(query_unit[:half_rows], plane_a), double(query_unit[half_rows:], plane_b)], axis=0
        ),
        [core],
    )
    positive_saved, positive_unit = tower_forward(positive_features, item_first, item_second, item_third)
    positive_wide = positive_unit.astype(f32)
    query_wide = query_unit.astype(f32)
    positive_logit = jnp.sum(query_wide * positive_wide, axis=1) * inv_temp - jnp.log(
        positive_counts.astype(f32)
    )
    positive_exp = jnp.exp(positive_logit)

    scores = contract_cols(group_unit, shard_unit) * inv_temp - shard_log[None, :]
    weights = jnp.where(group_ids[:, None] != shard_ids[None, :], jnp.exp(scores), 0.0)
    block = weights.astype(bf16)
    denom = jnp.sum(weights, axis=1).reshape(len(blocks), half_rows)
    second_block = len(keys_a)
    own_exp = jnp.zeros_like(denom)
    own_exp = own_exp.at[0].set(positive_exp[:half_rows]).at[second_block].set(positive_exp[half_rows:])
    denom = denom + own_exp
    for mask in [core] + plane_a:
        other = swap(denom, mask)
        denom = denom + jnp.concatenate(
            [other[i : i + 1] for i in (blocks.index((c, k ^ mask)) for c, k in blocks)], axis=0
        )
    own_denom = jnp.concatenate([denom[0], denom[second_block]])
    query_part = jnp.dot(block, shard_unit, preferred_element_type=f32)
    query_part = halve(query_part, [core])
    cut = second_block * half_rows
    query_sum = jnp.concatenate(
        [halve(query_part[:cut], plane_a), halve(query_part[cut:], plane_b)], axis=0
    )
    loss_part = jnp.sum(jnp.log(own_denom) - positive_logit)
    positive_slope = positive_exp / own_denom - 1.0
    query_grad = (query_sum / own_denom[:, None] + positive_slope[:, None] * positive_wide) * inv_temp
    positive_grad = positive_slope[:, None] * query_wide * inv_temp

    scaled_unit = (group_unit.astype(f32) / denom.reshape(-1)[:, None]).astype(bf16)
    negative_part = contract_rows(block, scaled_unit)
    cut = half_negs * (dps // 2)
    negative_sum = jnp.concatenate(
        [halve(negative_part[:cut], line_a), halve(negative_part[cut:], line_b)], axis=0
    )

    def pack(gradients):
        first, second, third = gradients
        width = third.shape[1]
        first = first.reshape(devices, -1, first.shape[1])
        cols = [second[:, at : at + width] for at in range(0, second.shape[1], width)] + [third]
        rest = jnp.concatenate([c.reshape(devices, -1, width) for c in cols], axis=1)
        return [a.reshape((2,) * bits + a.shape[1:]) for a in (first, rest)]

    order_a = list(range(bits))
    order_b = [0, neg_bits] + [b for b in range(1, bits) if b != neg_bits]

    def reduce_grads(gradients):
        first, rest = pack(gradients)
        return scatter_sum(first, bits, order_a, flat), scatter_sum(rest, bits, order_b, flat)

    query_grads = tower_backward(query_features, query_second, query_third, query_saved, query_grad)
    query_first_sum, query_rest_sum = reduce_grads(query_grads)
    positive_grads = tower_backward(
        positive_features, item_second, item_third, positive_saved, positive_grad
    )
    negative_grads = tower_backward(
        negative_features, item_second, item_third, negative_saved, negative_sum * inv_temp
    )
    item_grads = tuple(p + n for p, n in zip(positive_grads, negative_grads))
    item_first_sum, item_rest_sum = reduce_grads(item_grads)

    pieces = (query_first_sum, query_rest_sum, item_first_sum, item_rest_sum)
    squares = sum(jnp.sum(piece * piece) for piece in pieces)
    lane = lax.broadcasted_iota(jnp.int32, (8, 128), 1)
    totals = jnp.where(lane == 0, squares, jnp.where(lane == 1, loss_part, 0.0))
    for bit in range(bits):
        totals = totals + swap(totals, 1 << bit)
    mean_loss = totals[0, 1] / (own_rows * devices)
    grad_norm = jnp.sqrt(totals[0, 0])
    clip_factor = clip_norm / jnp.maximum(grad_norm, clip_norm)

    def spread(pair):
        value = jnp.stack(pair, 0).astype(bf16)[None]
        for bit in list(range(1, neg_bits)) + [0]:
            other = swap(value, 1 << bit)
            own = ((flat >> bit) & 1) != 0
            low, high = jnp.where(own, other, value), jnp.where(own, value, other)
            if bit == 0:
                value = jnp.stack([low, high], 1)
            else:
                value = jnp.concatenate([low, high], 0)
        value = value.reshape((negs,) + value.shape[2:])
        return value.astype(f32) * clip_factor

    firsts = spread((query_first_sum, item_first_sum))
    rests = spread((query_rest_sum, item_rest_sum))

    def unpack(which, gradients):
        first, second, third = gradients
        width = third.shape[1]
        clipped_first = firsts[:, which].reshape(-1, first.shape[1])
        rest = rests[:, which]
        height = second.shape[0] // devices
        count = second.shape[1] // width
        cols = [rest[:, i * height : (i + 1) * height].reshape(-1, width) for i in range(count)]
        clipped_second = jnp.concatenate(cols, axis=1)
        clipped_third = rest[:, count * height :].reshape(-1, width)
        return (clipped_first, clipped_second, clipped_third)

    return (mean_loss,) + unpack(0, query_grads) + unpack(1, item_grads)


def solution(mesh):
    placed = (
        P(("dp", "neg"), None),
        P(("dp", "neg"), None),
        P(("neg", "dp"), None),
        P("dp"),
        P(("dp", "neg")),
        P("neg"),
        P("neg"),
        P(),
        P(),
        P(),
        P(),
        P(),
        P(),
    )
    return jax.shard_map(
        per_device,
        mesh=mesh,
        in_specs=placed,
        out_specs=(
            P(),
            P("dp", None),
            P("dp", None),
            P("dp", None),
            P("dp", None),
            P("dp", None),
            P("dp", None),
        ),
        check_vma=False,
    )
```
